256 devices in a mesh: tm: 8 (over y, x_lo), rows: 32 (over x_hi, z, core).
Axes of the slice: x: 4 (x_hi: 2, x_lo: 2; x = x_hi * 2 + x_lo), y: 4, z: 8, core: 2. Of those that a mesh axis runs over, the one named last changes fastest.
Arguments:
- queries: bfloat16 [32, 256, 16, 1792], P('tm', 'rows'), may hold values from -60 to 60
- keys: bfloat16 [32, 256, 16, 1792], P('tm', 'rows'), may hold values from -6 to 6
- values: bfloat16 [32, 256, 16, 1792], P('tm', 'rows'), may hold values from -6 to 6
- out_grad: bfloat16 [32, 256, 16, 1792], P('tm', 'rows'), may hold values from -6 to 6
Outputs:
- query_grad: bfloat16 [32, 256, 16, 1792], P('tm', 'rows')
- key_grad: bfloat16 [32, 256, 16, 1792], P('tm', 'rows')
- value_grad: bfloat16 [32, 256, 16, 1792], P('tm', 'rows')
The draws below stay inside these ranges and needn't reach their ends.
All inputs are finite; a program needn't handle non-finite values.
Results may differ from the reference program's by a relative error of at most 0.012.
Values may be sent and summed in bfloat16 or wider, within the bound.
A program may use at most 128 MiB of HBM per device.

```python
import math
import jax
import jax.numpy as jnp
from jax import lax

WT = 4
WH = 8
WW = 8
HEADS = 14
HEAD_DIM = 128
COLS = 16
FRAMES = 32
ROWS = 256


def paired_fields(key):
    base = jax.random.fold_in(key, 17)
    key_query, key_key = jax.random.split(base, 2)
    shape = (FRAMES, ROWS, COLS, HEADS, HEAD_DIM)
    query_field = jnp.clip(jax.random.normal(key_query, shape, jnp.float32), -6.0, 6.0)
    key_field = jnp.clip(jax.random.normal(key_key, shape, jnp.float32), -6.0, 6.0)
    query_field = query_field.reshape(FRAMES, ROWS, COLS, HEADS * HEAD_DIM)
    key_field = key_field.reshape(FRAMES, ROWS, COLS, HEADS * HEAD_DIM)
    return (query_field, key_field)


def draw_queries(key, part):
    return paired_fields(key)[0].astype(jnp.bfloat16)


def draw_keys(key, part):
    return paired_fields(key)[1].astype(jnp.bfloat16)


def steps_of(key, dims, cuts, smallest, top_value):
    factor_of = 1.0
    for position, blocks in cuts:
        heights = jax.random.uniform(jax.random.fold_in(jax.random.fold_in(key, 6), position), (blocks,), jnp.float32, smallest / len(cuts), top_value / len(cuts))
        factor_of = factor_of * jnp.repeat(jnp.exp(heights), dims[position] // blocks).reshape((-1,) + (1,) * (len(dims) - 1 - position))
    return factor_of


def scatter_about(stream_key, extent, width, most, cuts=(), kind=jnp.bfloat16):
    values = jax.random.normal(stream_key, extent, jnp.float32) * width
    if len(cuts) > 0:
        values = steps_of(stream_key, extent, cuts, -0.22, 0.18) * values
    return jnp.clip(values, min=-most, max=most).astype(kind)


def setup_inputs(seed: int = 0) -> dict:
    key_of = jax.random.split(jax.random.key(seed), 5)
    return {
        "queries": draw_queries(jax.random.fold_in(key_of[4], 71), 0),
        "keys": draw_keys(jax.random.fold_in(key_of[4], 71), 0),
        "values": scatter_about(key_of[2], (FRAMES, ROWS, COLS, HEADS * HEAD_DIM), 1.0, 6.0, ((0, 8), (1, 32))),
        "out_grad": scatter_about(key_of[3], (FRAMES, ROWS, COLS, HEADS * HEAD_DIM), 1.0, 6.0, ((0, 8), (1, 32))),
    }


def window_grads(query_w, key_w, value_w, grad_w):
    factor = 1.0 / math.sqrt(query_w.shape[-1])
    query_f = query_w.astype(jnp.float32)
    key_f = key_w.astype(jnp.float32)
    value_f = value_w.astype(jnp.float32)
    grad_f = grad_w.astype(jnp.float32)
    scores = jnp.einsum('bhqd,bhkd->bhqk', query_f, key_f) * factor
    weights = jax.nn.softmax(scores, axis=-1)
    weights_b = weights.astype(jnp.bfloat16)
    weights_bf = weights_b.astype(jnp.float32)
    attended = jnp.einsum('bhqk,bhkd->bhqd', weights_bf, value_f)
    row_dot = lax.optimization_barrier(jnp.sum(grad_f * attended, axis=-1, keepdims=True))
    weight_grad = jnp.einsum('bhqd,bhkd->bhqk', grad_f, value_f)
    score_grad = (weights * (weight_grad - row_dot) * factor).astype(jnp.bfloat16).astype(jnp.float32)
    value_out = jnp.einsum('bhqk,bhqd->bhkd', weights_bf, grad_f).astype(jnp.bfloat16)
    query_out = jnp.einsum('bhqk,bhkd->bhqd', score_grad, key_f).astype(jnp.bfloat16)
    key_out = jnp.einsum('bhqk,bhqd->bhkd', score_grad, query_f).astype(jnp.bfloat16)
    return jnp.stack((query_out, key_out, value_out))

def reference(queries, keys, values, out_grad):
    total_frames, total_rows, columns, features = queries.shape
    slabs = total_frames // WT
    window_count = columns // WW
    row_windows = total_rows // WH
    length = WT * WH * WW

    def slab_grads(index):
        frame_ids = (index * WT + WT // 2 + jnp.arange(WT, dtype=jnp.int32)) % total_frames

        def prepare(field):
            piece = jnp.take(field, frame_ids, axis=0)
            piece = jnp.roll(piece, (-(WH // 2), -(WW // 2)), axis=(1, 2))
            piece = piece.reshape(WT, row_windows, WH, window_count, WW, HEADS, HEAD_DIM)
            return piece.transpose(1, 3, 5, 0, 2, 4, 6).reshape(row_windows, window_count, HEADS, length, HEAD_DIM)
        inputs = tuple((prepare(field) for field in (queries, keys, values, out_grad)))
        grads = lax.map(lambda group: window_grads(group[0], group[1], group[2], group[3]), inputs)
        grads = grads.reshape(row_windows, 3, window_count, HEADS, WT, WH, WW, HEAD_DIM)
        grads = grads.transpose(1, 4, 0, 5, 2, 6, 3, 7).reshape(3, WT, total_rows, columns, features)
        return jnp.roll(grads, (WH // 2, WW // 2), axis=(2, 3))
    stacked = lax.map(slab_grads, jnp.arange(slabs, dtype=jnp.int32))
    stacked = stacked.transpose(1, 0, 2, 3, 4, 5).reshape(3, total_frames, total_rows, columns, features)
    stacked = jnp.roll(stacked, WT // 2, axis=1)
    return (stacked[0], stacked[1], stacked[2])
```

```python
import functools
import math

import jax
import jax.numpy as jnp
from jax import lax
from jax.experimental import pallas as pl
from jax.experimental.pallas import tpu as pltpu
from jax.sharding import PartitionSpec as P

MESH = pl.DeviceIdType.MESH
HEAD_DIM = 128
WW = 8
AHEAD = 3
LAG = 3

PER_HALF = 12
OWN_ROLE = (2, 0)


def kernel(tm, rows, q_ref, k_ref, v_ref, g_ref, dq_ref, dk_ref, dv_ref, blocks, stat_out, stat_in, dq_part, dkv,
           dq_in, dq_sum, sems):
    t, r = lax.axis_index("tm"), lax.axis_index("rows")
    frames, rows_here, cols, features = q_ref.shape
    heads = features // HEAD_DIM
    fh, rh = frames // 2, rows_here // 2
    factor = 1.0 / math.sqrt(HEAD_DIM)
    side = rows // 2
    seam_before = 1 - (r % side + side - 1) // side
    seam_after = 1 - ((r + 1) % side + side - 1) // side
    tp, tn = (t + 1) % tm, (t + tm - 1) % tm
    rp, rn = (r + 1) % rows, (r + rows - 1) % rows

    (fwd_send, fwd_recv, load_sem, stat_send, stat_recv, out_send, dq_recv, dkv_recv, dkv_store, dq_store) = (
        sems.at[i] for i in range(10)
    )

    def quad(ref, late_frames, late_rows, h):
        return ref.at[
            pl.ds(late_frames * fh, fh),
            pl.ds(late_rows * rh, rh),
            :,
            pl.ds(pl.multiple_of(h * HEAD_DIM, HEAD_DIM), HEAD_DIM),
        ]

    def send(src, dst, send_sem, recv_sem, device):
        pltpu.make_async_remote_copy(
            src_ref=src, dst_ref=dst, send_sem=send_sem, recv_sem=recv_sem, device_id=device, device_id_type=MESH
        ).start()

    def wait_bytes(ref, sem):
        pltpu.make_async_copy(ref, ref, sem).wait()

    barrier = pltpu.get_barrier_semaphore()
    around = [(tp, r), (tn, r), (t, rp), (t, rn), (tp, rp), (tp, rn), (tn, rp), (tn, rn)]
    for device in around:
        pl.semaphore_signal(barrier, inc=1, device_id=device, device_id_type=MESH)

    def load_own(h, carry):
        for half in range(2):
            base = half * PER_HALF
            role = OWN_ROLE[half]
            for ref, slot in ((q_ref, role), (g_ref, 4 + role), (k_ref, 8), (v_ref, 10)):
                pltpu.make_async_copy(quad(ref, half, 1, h), blocks.at[h, base + slot], load_sem.at[h]).start()
        return carry

    lax.fori_loop(0, heads, load_own, 0)
    pl.semaphore_wait(barrier, len(around))

    def send_inputs(h):
        sem = (fwd_send.at[h], fwd_recv.at[h])
        for ref, off in ((q_ref, 0), (g_ref, 4)):
            send(quad(ref, 1, 1, h), blocks.at[h, off + 0], *sem, (tp, r))
            send(quad(ref, 0, 1, h), blocks.at[h, PER_HALF + off + 2], *sem, (tn, r))
            send(quad(ref, 1, 0, h), blocks.at[h, off + 1], *sem, (tp, rn))
            send(quad(ref, 0, 0, h), blocks.at[h, PER_HALF + off + 3], *sem, (tn, rn))
            send(quad(ref, 1, 0, h), blocks.at[h, PER_HALF + off + 1], *sem, (t, rn))
            send(quad(ref, 0, 0, h), blocks.at[h, off + 3], *sem, (t, rn))
        for ref, off in ((k_ref, 9), (v_ref, 11)):
            send(
                quad(ref, 1, 0, h),
                blocks.at[h, (1 - seam_before) * PER_HALF + off],
                *sem,
                ((t + seam_before) % tm, rn),
            )
            send(
                quad(ref, 0, 0, h),
                blocks.at[h, seam_before * PER_HALF + off],
                *sem,
                ((t + tm - seam_before) % tm, rn),
            )

    def send_stats(h):
        sem = (stat_send.at[h], stat_recv.at[h])
        send(stat_out.at[h, 1], stat_in.at[h, 0], *sem, (tp, r))
        send(stat_out.at[h, 0], stat_in.at[h, 1], *sem, (tn, r))

    def send_outputs(h):
        sem = (out_send.at[h], dq_recv.at[h])
        send(dq_part.at[h, 1, 2], dq_in.at[h, 5], *sem, (tp, r))
        send(dq_part.at[h, 0, 0], dq_in.at[h, 4], *sem, (tn, r))
        send(dq_part.at[h, 1, 3], dq_in.at[h, 2], *sem, (tp, rp))
        send(dq_part.at[h, 0, 1], dq_in.at[h, 1], *sem, (tn, rp))
        send(dq_part.at[h, 1, 1], dq_in.at[h, 0], *sem, (t, rp))
        send(dq_part.at[h, 0, 3], dq_in.at[h, 3], *sem, (t, rp))
        sem = (out_send.at[h], dkv_recv.at[h])
        for kind, ref in enumerate((dk_ref, dv_ref)):
            send(
                dkv.at[h, kind, 1, 1], quad(ref, 1 - seam_after, 0, h), *sem, ((t + seam_after) % tm, rp)
            )
            send(
                dkv.at[h, kind, 0, 1], quad(ref, seam_after, 0, h), *sem, ((t + tm - seam_after) % tm, rp)
            )
            for half in range(2):
                pltpu.make_async_copy(dkv.at[h, kind, half, 0], quad(ref, half, 1, h), dkv_store.at[h]).start()

    key_col = lax.broadcasted_iota(jnp.int32, (cols, HEAD_DIM), 0)
    query_col = lax.broadcasted_iota(jnp.int32, (cols, HEAD_DIM), 1)
    shifted = cols - WW // 2
    apart = ((key_col + shifted) ^ (query_col + shifted)) & WW
    bias = jnp.where(apart == 0, 0.0, -1e30).astype(jnp.float32)

    tokens = fh * rh * cols

    def block(h, index, count=1):
        return blocks[h, pl.ds(index, count)].reshape(count * tokens, HEAD_DIM)

    def scores_of(keys, queries):
        scores = lax.dot_general(keys, queries, (((1,), (1,)), ((), ())), preferred_element_type=jnp.float32)
        scores = (scores * factor).reshape(2 * tokens // cols, cols, tokens) + bias[None]
        return scores.reshape(2 * tokens, tokens)

    def first_stage(h):
        for half in range(2):
            base = half * PER_HALF
            keys, values = block(h, base + 8, 2), block(h, base + 10, 2)
            for role in range(4):
                scores = scores_of(keys, block(h, base + role))
                dprobs = lax.dot_general(
                    values, block(h, base + 4 + role), (((1,), (1,)), ((), ())), preferred_element_type=jnp.float32
                )
                top = jnp.max(scores, axis=0, keepdims=True)
                weights = jnp.exp(scores - top)
                total = jnp.sum(weights, axis=0, keepdims=True)
                dots = jnp.sum(weights * dprobs, axis=0, keepdims=True)
                lanes = pl.ds(role * tokens, tokens)
                stat_out[h, half, 0:1, lanes] = top + jnp.log(total)
                stat_out[h, half, 1:2, lanes] = dots / total

    def second_stage(h):
        for half in range(2):
            base = half * PER_HALF
            keys, values = block(h, base + 8, 2), block(h, base + 10, 2)
            dk = jnp.zeros((2 * tokens, HEAD_DIM), jnp.float32)
            dv = jnp.zeros((2 * tokens, HEAD_DIM), jnp.float32)
            for role in range(4):
                lanes = pl.ds(role * tokens, tokens)
                mine, other = stat_out[h, half, 0:1, lanes], stat_in[h, half, 0:1, lanes]
                norm = jnp.maximum(mine, other) + jnp.log(1.0 + jnp.exp(-jnp.abs(mine - other)))
                row_dot = stat_out[h, half, 1:2, lanes] * jnp.exp(mine - norm)
                row_dot += stat_in[h, half, 1:2, lanes] * jnp.exp(other - norm)
                queries, grads = block(h, base + role), block(h, base + 4 + role)
                probs = jnp.exp(scores_of(keys, queries) - norm)
                dprobs = lax.dot_general(
                    values, grads, (((1,), (1,)), ((), ())), preferred_element_type=jnp.float32
                )
                dscores = (probs * (dprobs - row_dot) * factor).astype(jnp.bfloat16)
                dv += jnp.dot(probs.astype(jnp.bfloat16), grads, preferred_element_type=jnp.float32)
                dk += jnp.dot(dscores, queries, preferred_element_type=jnp.float32)
                dq = lax.dot_general(dscores, keys, (((0,), (0,)), ((), ())), preferred_element_type=jnp.float32)
                dq_part[h, half, role] = dq.astype(jnp.bfloat16).reshape(fh, rh, cols, HEAD_DIM)
            dkv[h, 0, half] = dk.astype(jnp.bfloat16).reshape(2, fh, rh, cols, HEAD_DIM)
            dkv[h, 1, half] = dv.astype(jnp.bfloat16).reshape(2, fh, rh, cols, HEAD_DIM)

    for h in range(min(AHEAD, heads)):
        send_inputs(h)

    def step(i, carry):
        @pl.when(i < heads)
        def _():
            wait_bytes(blocks.at[i, pl.ds(0, 8)], load_sem.at[i])
            wait_bytes(blocks.at[i, pl.ds(0, 16)], fwd_recv.at[i])

        @pl.when(i + AHEAD < heads)
        def _():
            send_inputs(i + AHEAD)

        @pl.when(i > LAG)
        def _():
            send_outputs(i - LAG - 1)

        @pl.when(i < heads)
        def _():
            first_stage(i)

        @pl.when((i >= LAG) & (i < heads + LAG))
        def _():
            wait_bytes(stat_in.at[i - LAG], stat_recv.at[i - LAG])
            second_stage(i - LAG)

        @pl.when(i < heads)
        def _():
            send_stats(i)

        return carry

    lax.fori_loop(0, heads + LAG + 1, step, 0)

    def finish(h, carry):
        wait_bytes(dq_in.at[h], dq_recv.at[h])
        f32 = jnp.float32
        dq_sum[h, 1, 0] = (dq_in[h, 0].astype(f32) + dq_in[h, 1].astype(f32)).astype(jnp.bfloat16)
        dq_sum[h, 0, 0] = (dq_in[h, 2].astype(f32) + dq_in[h, 3].astype(f32)).astype(jnp.bfloat16)
        dq_sum[h, 1, 1] = (dq_in[h, 4].astype(f32) + dq_part[h, 1, 0].astype(f32)).astype(jnp.bfloat16)
        dq_sum[h, 0, 1] = (dq_in[h, 5].astype(f32) + dq_part[h, 0, 2].astype(f32)).astype(jnp.bfloat16)
        for half in range(2):
            for late_rows in range(2):
                pltpu.make_async_copy(
                    dq_sum.at[h, half, late_rows], quad(dq_ref, half, late_rows, h), dq_store.at[h]
                ).start()
        return carry

    lax.fori_loop(0, heads, finish, 0)

    def drain(h, carry):
        wait_bytes(blocks.at[h, pl.ds(0, 16)], fwd_send.at[h])
        wait_bytes(stat_out.at[h], stat_send.at[h])
        wait_bytes(blocks.at[h, pl.ds(0, 10)], out_send.at[h])
        wait_bytes(blocks.at[h, pl.ds(0, 4)], dkv_recv.at[h])
        wait_bytes(blocks.at[h, pl.ds(0, 4)], dkv_store.at[h])
        wait_bytes(blocks.at[h, pl.ds(0, 4)], dq_store.at[h])
        return carry

    lax.fori_loop(0, heads, drain, 0)


def solution(mesh):
    tm, rows = mesh.shape["tm"], mesh.shape["rows"]

    def shards(queries, keys, values, out_grad):
        frames, rows_here, cols, features = queries.shape
        heads = features // HEAD_DIM
        fh, rh = frames // 2, rows_here // 2
        tokens = fh * rh * cols
        quadrant = (fh, rh, cols, HEAD_DIM)
        bf16 = jnp.bfloat16
        hbm = pl.BlockSpec(memory_space=pl.ANY)
        out = jax.ShapeDtypeStruct(queries.shape, bf16)
        return pl.pallas_call(
            functools.partial(kernel, tm, rows),
            out_shape=(out, out, out),
            in_specs=[hbm] * 4,
            out_specs=(hbm, hbm, hbm),
            scratch_shapes=[
                pltpu.VMEM((heads, 2 * PER_HALF, *quadrant), bf16),
                pltpu.VMEM((heads, 2, 2, 4 * tokens), jnp.float32),
                pltpu.VMEM((heads, 2, 2, 4 * tokens), jnp.float32),
                pltpu.VMEM((heads, 2, 4, *quadrant), bf16),
                pltpu.VMEM((heads, 2, 2, 2, *quadrant), bf16),
                pltpu.VMEM((heads, 6, *quadrant), bf16),
                pltpu.VMEM((heads, 2, 2, *quadrant), bf16),
                pltpu.SemaphoreType.DMA((10, heads)),
            ],
            compiler_params=pltpu.CompilerParams(
                collective_id=0, has_side_effects=True, vmem_limit_bytes=60 * 1024 * 1024
            ),
        )(queries, keys, values, out_grad)

    spec = P("tm", "rows", None, None)
    return jax.shard_map(
        shards, mesh=mesh, in_specs=(spec,) * 4, out_specs=(spec,) * 3, check_vma=False
    )
```

```python
import functools
import math

import jax
import jax.numpy as jnp
from jax import lax
from jax.experimental import pallas as pl
from jax.experimental.pallas import tpu as pltpu
from jax.sharding import PartitionSpec as P

MESH = pl.DeviceIdType.MESH
HEAD_DIM = 128
WW = 8
AHEAD = 3
LAG = 3

PER_HALF = 12
OWN_ROLE = (2, 0)


def kernel(tm, rows, q_ref, k_ref, v_ref, g_ref, dq_ref, dk_ref, dv_ref, blocks, stat_out, stat_in, dq_part, dkv,
           dq_in, sems):
    t, r = lax.axis_index("tm"), lax.axis_index("rows")
    frames, rows_here, cols, features = q_ref.shape
    heads = features // HEAD_DIM
    fh, rh = frames // 2, rows_here // 2
    factor = 1.0 / math.sqrt(HEAD_DIM)
    side = rows // 2
    seam_before = 1 - (r % side + side - 1) // side
    seam_after = 1 - ((r + 1) % side + side - 1) // side
    tp, tn = (t + 1) % tm, (t + tm - 1) % tm
    rp, rn = (r + 1) % rows, (r + rows - 1) % rows

    (fwd_send, fwd_recv, load_sem, stat_send, stat_recv, out_send, dq_recv, dkv_recv) = (
        sems.at[i] for i in range(8)
    )

    def quad(ref, late_frames, late_rows, h):
        return ref.at[
            pl.ds(late_frames * fh, fh),
            pl.ds(late_rows * rh, rh),
            :,
            pl.ds(pl.multiple_of(h * HEAD_DIM, HEAD_DIM), HEAD_DIM),
        ]

    def put(ref, late_frames, late_rows, h, value):
        lanes = pl.ds(pl.multiple_of(h * HEAD_DIM, HEAD_DIM), HEAD_DIM)
        ref[pl.ds(late_frames * fh, fh), pl.ds(late_rows * rh, rh), :, lanes] = value

    def send(src, dst, send_sem, recv_sem, device):
        pltpu.make_async_remote_copy(
            src_ref=src, dst_ref=dst, send_sem=send_sem, recv_sem=recv_sem, device_id=device, device_id_type=MESH
        ).start()

    def wait_bytes(ref, sem):
        pltpu.make_async_copy(ref, ref, sem).wait()

    barrier = pltpu.get_barrier_semaphore()
    around = [(tp, r), (tn, r), (t, rp), (t, rn), (tp, rp), (tp, rn), (tn, rp), (tn, rn)]
    for device in around:
        pl.semaphore_signal(barrier, inc=1, device_id=device, device_id_type=MESH)

    def load_own(h, carry):
        for half in range(2):
            base = half * PER_HALF
            role = OWN_ROLE[half]
            for ref, slot in ((q_ref, role), (g_ref, 4 + role), (k_ref, 8), (v_ref, 10)):
                pltpu.make_async_copy(quad(ref, half, 1, h), blocks.at[h, base + slot], load_sem.at[h]).start()
        return carry

    lax.fori_loop(0, heads, load_own, 0)
    pl.semaphore_wait(barrier, len(around))

    def send_inputs(h):
        sem = (fwd_send.at[h], fwd_recv.at[h])
        for ref, off in ((q_ref, 0), (g_ref, 4)):
            send(quad(ref, 1, 1, h), blocks.at[h, off + 0], *sem, (tp, r))
            send(quad(ref, 0, 1, h), blocks.at[h, PER_HALF + off + 2], *sem, (tn, r))
            send(quad(ref, 1, 0, h), blocks.at[h, off + 1], *sem, (tp, rn))
            send(quad(ref, 0, 0, h), blocks.at[h, PER_HALF + off + 3], *sem, (tn, rn))
            send(quad(ref, 1, 0, h), blocks.at[h, PER_HALF + off + 1], *sem, (t, rn))
            send(quad(ref, 0, 0, h), blocks.at[h, off + 3], *sem, (t, rn))
        for ref, off in ((k_ref, 9), (v_ref, 11)):
            send(
                quad(ref, 1, 0, h),
                blocks.at[h, (1 - seam_before) * PER_HALF + off],
                *sem,
                ((t + seam_before) % tm, rn),
            )
            send(
                quad(ref, 0, 0, h),
                blocks.at[h, seam_before * PER_HALF + off],
                *sem,
                ((t + tm - seam_before) % tm, rn),
            )

    def send_stats(h):
        sem = (stat_send.at[h], stat_recv.at[h])
        send(stat_out.at[h, 1], stat_in.at[h, 0], *sem, (tp, r))
        send(stat_out.at[h, 0], stat_in.at[h, 1], *sem, (tn, r))

    def send_outputs(h):
        sem = (out_send.at[h], dq_recv.at[h])
        send(dq_part.at[h, 1, 2], dq_in.at[h, 5], *sem, (tp, r))
        send(dq_part.at[h, 0, 0], dq_in.at[h, 4], *sem, (tn, r))
        send(dq_part.at[h, 1, 3], dq_in.at[h, 2], *sem, (tp, rp))
        send(dq_part.at[h, 0, 1], dq_in.at[h, 1], *sem, (tn, rp))
        send(dq_part.at[h, 1, 1], dq_in.at[h, 0], *sem, (t, rp))
        send(dq_part.at[h, 0, 3], dq_in.at[h, 3], *sem, (t, rp))
        sem = (out_send.at[h], dkv_recv.at[h])
        for kind, ref in enumerate((dk_ref, dv_ref)):
            send(dkv.at[h, kind, 1], quad(ref, 1 - seam_after, 0, h), *sem, ((t + seam_after) % tm, rp))
            send(dkv.at[h, kind, 0], quad(ref, seam_after, 0, h), *sem, ((t + tm - seam_after) % tm, rp))

    key_col = lax.broadcasted_iota(jnp.int32, (cols, HEAD_DIM), 0)
    query_col = lax.broadcasted_iota(jnp.int32, (cols, HEAD_DIM), 1)
    shifted = cols - WW // 2
    apart = ((key_col + shifted) ^ (query_col + shifted)) & WW
    bias = jnp.where(apart == 0, 0.0, -1e30).astype(jnp.float32)

    tokens = fh * rh * cols

    def block(h, index, count=1):
        return blocks[h, pl.ds(index, count)].reshape(count * tokens, HEAD_DIM)

    def scores_of(keys, queries):
        scores = lax.dot_general(keys, queries, (((1,), (1,)), ((), ())), preferred_element_type=jnp.float32)
        scores = (scores * factor).reshape(2 * tokens // cols, cols, tokens) + bias[None]
        return scores.reshape(2 * tokens, tokens)

    def first_stage(h):
        for half in range(2):
            base = half * PER_HALF
            keys, values = block(h, base + 8, 2), block(h, base + 10, 2)
            for role in range(4):
                scores = scores_of(keys, block(h, base + role))
                dprobs = lax.dot_general(
                    values, block(h, base + 4 + role), (((1,), (1,)), ((), ())), preferred_element_type=jnp.float32
                )
                top = jnp.max(scores, axis=0, keepdims=True)
                weights = jnp.exp(scores - top)
                total = jnp.sum(weights, axis=0, keepdims=True)
                dots = jnp.sum(weights * dprobs, axis=0, keepdims=True)
                lanes = pl.ds(role * tokens, tokens)
                stat_out[h, half, 0:1, lanes] = top + jnp.log(total)
                stat_out[h, half, 1:2, lanes] = dots / total

    def second_stage(h):
        for half in range(2):
            base = half * PER_HALF
            keys, values = block(h, base + 8, 2), block(h, base + 10, 2)
            dk = jnp.zeros((2 * tokens, HEAD_DIM), jnp.float32)
            dv = jnp.zeros((2 * tokens, HEAD_DIM), jnp.float32)
            for role in range(4):
                lanes = pl.ds(role * tokens, tokens)
                mine, other = stat_out[h, half, 0:1, lanes], stat_in[h, half, 0:1, lanes]
                norm = jnp.maximum(mine, other) + jnp.log(1.0 + jnp.exp(-jnp.abs(mine - other)))
                row_dot = stat_out[h, half, 1:2, lanes] * jnp.exp(mine - norm)
                row_dot += stat_in[h, half, 1:2, lanes] * jnp.exp(other - norm)
                queries, grads = block(h, base + role), block(h, base + 4 + role)
                probs = jnp.exp(scores_of(keys, queries) - norm)
                dprobs = lax.dot_general(
                    values, grads, (((1,), (1,)), ((), ())), preferred_element_type=jnp.float32
                )
                dscores = (probs * (dprobs - row_dot) * factor).astype(jnp.bfloat16)
                dv += jnp.dot(probs.astype(jnp.bfloat16), grads, preferred_element_type=jnp.float32)
                dk += jnp.dot(dscores, queries, preferred_element_type=jnp.float32)
                dq = lax.dot_general(dscores, keys, (((0,), (0,)), ((), ())), preferred_element_type=jnp.float32)
                dq_part[h, half, role] = dq.astype(jnp.bfloat16).reshape(fh, rh, cols, HEAD_DIM)
            for kind, (ref, total) in enumerate(((dk_ref, dk), (dv_ref, dv))):
                total = total.astype(jnp.bfloat16).reshape(2, fh, rh, cols, HEAD_DIM)
                put(ref, half, 1, h, total[0])
                dkv[h, kind, half] = total[1]

    for h in range(min(AHEAD, heads)):
        send_inputs(h)

    def step(i, carry):
        @pl.when(i < heads)
        def _():
            wait_bytes(blocks.at[i, pl.ds(0, 8)], load_sem.at[i])
            wait_bytes(blocks.at[i, pl.ds(0, 16)], fwd_recv.at[i])

        @pl.when(i + AHEAD < heads)
        def _():
            send_inputs(i + AHEAD)

        @pl.when(i > LAG)
        def _():
            send_outputs(i - LAG - 1)

        @pl.when(i < heads)
        def _():
            first_stage(i)

        @pl.when((i >= LAG) & (i < heads + LAG))
        def _():
            wait_bytes(stat_in.at[i - LAG], stat_recv.at[i - LAG])
            second_stage(i - LAG)

        @pl.when(i < heads)
        def _():
            send_stats(i)

        return carry

    lax.fori_loop(0, heads + LAG + 1, step, 0)

    def finish(h, carry):
        wait_bytes(dq_in.at[h], dq_recv.at[h])
        own = dq_part.at[h]
        for half, late_rows, first, second in (
            (1, 0, dq_in.at[h, 0], dq_in.at[h, 1]),
            (0, 0, dq_in.at[h, 2], dq_in.at[h, 3]),
            (1, 1, dq_in.at[h, 4], own.at[1, 0]),
            (0, 1, dq_in.at[h, 5], own.at[0, 2]),
        ):
            total = first[...].astype(jnp.float32) + second[...].astype(jnp.float32)
            put(dq_ref, half, late_rows, h, total.astype(jnp.bfloat16))
        return carry

    lax.fori_loop(0, heads, finish, 0)

    def drain(h, carry):
        wait_bytes(blocks.at[h, pl.ds(0, 16)], fwd_send.at[h])
        wait_bytes(stat_out.at[h], stat_send.at[h])
        wait_bytes(blocks.at[h, pl.ds(0, 10)], out_send.at[h])
        wait_bytes(blocks.at[h, pl.ds(0, 4)], dkv_recv.at[h])
        return carry

    lax.fori_loop(0, heads, drain, 0)


def write_out(*refs):
    sources, targets, sem = refs[:3], refs[3:6], refs[6]
    copies = [pltpu.make_async_copy(*pair, sem.at[i]) for i, pair in enumerate(zip(sources, targets))]
    for copy in copies:
        copy.start()
    for copy in copies:
        copy.wait()


def solution(mesh):
    tm, rows = mesh.shape["tm"], mesh.shape["rows"]

    def shards(queries, keys, values, out_grad):
        frames, rows_here, cols, features = queries.shape
        heads = features // HEAD_DIM
        fh, rh = frames // 2, rows_here // 2
        tokens = fh * rh * cols
        quadrant = (fh, rh, cols, HEAD_DIM)
        bf16 = jnp.bfloat16
        hbm, vmem = pl.BlockSpec(memory_space=pl.ANY), pl.BlockSpec(memory_space=pltpu.VMEM)
        held = pltpu.VMEM(queries.shape, bf16)
        grads = pl.pallas_call(
            functools.partial(kernel, tm, rows),
            out_shape=(held, held, held),
            in_specs=[hbm] * 4,
            out_specs=(vmem, vmem, vmem),
            scratch_shapes=[
                pltpu.VMEM((heads, 2 * PER_HALF, *quadrant), bf16),
                pltpu.VMEM((heads, 2, 2, 4 * tokens), jnp.float32),
                pltpu.VMEM((heads, 2, 2, 4 * tokens), jnp.float32),
                pltpu.VMEM((heads, 2, 4, *quadrant), bf16),
                pltpu.VMEM((heads, 2, 2, *quadrant), bf16),
                pltpu.VMEM((heads, 6, *quadrant), bf16),
                pltpu.SemaphoreType.DMA((8, heads)),
            ],
            compiler_params=pltpu.CompilerParams(
                collective_id=0, has_side_effects=True, vmem_limit_bytes=57 * 1024 * 1024
            ),
        )(queries, keys, values, out_grad)
        out = jax.ShapeDtypeStruct(queries.shape, bf16)
        return pl.pallas_call(
            write_out,
            out_shape=(out, out, out),
            in_specs=[vmem] * 3,
            out_specs=(hbm, hbm, hbm),
            scratch_shapes=[pltpu.SemaphoreType.DMA((3,))],
            compiler_params=pltpu.CompilerParams(vmem_limit_bytes=4 * 1024 * 1024),
        )(*(pltpu.with_memory_space_constraint(grad, pltpu.VMEM) for grad in grads))

    spec = P("tm", "rows", None, None)
    return jax.shard_map(
        shards, mesh=mesh, in_specs=(spec,) * 4, out_specs=(spec,) * 3, check_vma=False
    )
```

```python
import functools
import math

import jax
import jax.numpy as jnp
from jax import lax
from jax.experimental import pallas as pl
from jax.experimental.pallas import tpu as pltpu
from jax.sharding import PartitionSpec as P

MESH = pl.DeviceIdType.MESH
HEAD_DIM = 128
WW = 8
AHEAD = 2
LAG = 5

PER_HALF = 12
OWN_ROLE = (2, 0)


def kernel(tm, rows, q_ref, k_ref, v_ref, g_ref, dq_ref, dk_ref, dv_ref, blocks, stat_out, stat_in, dq_part, dkv,
           dq_in, sems):
    t, r = lax.axis_index("tm"), lax.axis_index("rows")
    frames, rows_here, cols, features = q_ref.shape
    heads = features // HEAD_DIM
    fh, rh = frames // 2, rows_here // 2
    factor = 1.0 / math.sqrt(HEAD_DIM)
    side = rows // 2
    seam_before = 1 - (r % side + side - 1) // side
    seam_after = 1 - ((r + 1) % side + side - 1) // side
    tp, tn = (t + 1) % tm, (t + tm - 1) % tm
    rp, rn = (r + 1) % rows, (r + rows - 1) % rows

    (fwd_send, fwd_recv, load_sem, stat_send, stat_recv, out_send, dq_recv, dkv_recv) = (
        sems.at[i] for i in range(8)
    )

    def quad(ref, late_frames, late_rows, h):
        return ref.at[
            pl.ds(late_frames * fh, fh),
            pl.ds(late_rows * rh, rh),
            :,
            pl.ds(pl.multiple_of(h * HEAD_DIM, HEAD_DIM), HEAD_DIM),
        ]

    def put(ref, late_frames, late_rows, h, value):
        lanes = pl.ds(pl.multiple_of(h * HEAD_DIM, HEAD_DIM), HEAD_DIM)
        ref[pl.ds(late_frames * fh, fh), pl.ds(late_rows * rh, rh), :, lanes] = value

    def send(src, dst, send_sem, recv_sem, device):
        pltpu.make_async_remote_copy(
            src_ref=src, dst_ref=dst, send_sem=send_sem, recv_sem=recv_sem, device_id=device, device_id_type=MESH
        ).start()

    def wait_bytes(ref, sem):
        pltpu.make_async_copy(ref, ref, sem).wait()

    barrier = pltpu.get_barrier_semaphore()
    senders = [(tp, r), (tn, r), (t, rp), (tp, rp), (tn, rp)]
    for device in senders:
        pl.semaphore_signal(barrier, inc=1, device_id=device, device_id_type=MESH)

    def load_own(h, carry):
        for half in range(2):
            base = half * PER_HALF
            role = OWN_ROLE[half]
            for ref, slot in ((q_ref, role), (g_ref, 4 + role), (k_ref, 8), (v_ref, 10)):
                pltpu.make_async_copy(quad(ref, half, 1, h), blocks.at[h, base + slot], load_sem.at[h]).start()
        return carry

    lax.fori_loop(0, heads, load_own, 0)
    pl.semaphore_wait(barrier, len(senders))

    def send_inputs(h):
        sem = (fwd_send.at[h], fwd_recv.at[h])
        for ref, off in ((q_ref, 0), (g_ref, 4)):
            send(quad(ref, 1, 1, h), blocks.at[h, off + 0], *sem, (tp, r))
            send(quad(ref, 0, 1, h), blocks.at[h, PER_HALF + off + 2], *sem, (tn, r))
            send(quad(ref, 1, 0, h), blocks.at[h, off + 1], *sem, (tp, rn))
            send(quad(ref, 0, 0, h), blocks.at[h, PER_HALF + off + 3], *sem, (tn, rn))
            send(quad(ref, 1, 0, h), blocks.at[h, PER_HALF + off + 1], *sem, (t, rn))
            send(quad(ref, 0, 0, h), blocks.at[h, off + 3], *sem, (t, rn))
        for ref, off in ((k_ref, 9), (v_ref, 11)):
            send(
                quad(ref, 1, 0, h),
                blocks.at[h, (1 - seam_before) * PER_HALF + off],
                *sem,
                ((t + seam_before) % tm, rn),
            )
            send(
                quad(ref, 0, 0, h),
                blocks.at[h, seam_before * PER_HALF + off],
                *sem,
                ((t + tm - seam_before) % tm, rn),
            )

    def send_stats(h):
        sem = (stat_send.at[h], stat_recv.at[h])
        send(stat_out.at[h, 1], stat_in.at[h, 0], *sem, (tp, r))
        send(stat_out.at[h, 0], stat_in.at[h, 1], *sem, (tn, r))

    def send_outputs(h):
        sem = (out_send.at[h], dq_recv.at[h])
        send(dq_part.at[h, 1, 1], dq_in.at[h, 0], *sem, (t, rp))
        send(dq_part.at[h, 0, 3], dq_in.at[h, 3], *sem, (t, rp))
        send(dq_part.at[h, 1, 3], dq_in.at[h, 2], *sem, (tp, rp))
        send(dq_part.at[h, 0, 1], dq_in.at[h, 1], *sem, (tn, rp))
        send(dq_part.at[h, 1, 2], dq_in.at[h, 5], *sem, (tp, r))
        send(dq_part.at[h, 0, 0], dq_in.at[h, 4], *sem, (tn, r))
        sem = (out_send.at[h], dkv_recv.at[h])
        for kind, ref in enumerate((dk_ref, dv_ref)):
            send(dkv.at[h, kind, 1], quad(ref, 1 - seam_after, 0, h), *sem, ((t + seam_after) % tm, rp))
            send(dkv.at[h, kind, 0], quad(ref, seam_after, 0, h), *sem, ((t + tm - seam_after) % tm, rp))

    key_col = lax.broadcasted_iota(jnp.int32, (cols, HEAD_DIM), 0)
    query_col = lax.broadcasted_iota(jnp.int32, (cols, HEAD_DIM), 1)
    shifted = cols - WW // 2
    apart = ((key_col + shifted) ^ (query_col + shifted)) & WW
    bias = jnp.where(apart == 0, 0.0, -1e30).astype(jnp.float32)

    tokens = fh * rh * cols

    def block(h, index, count=1):
        return blocks[h, pl.ds(index, count)].reshape(count * tokens, HEAD_DIM)

    def scores_of(keys, queries):
        scores = lax.dot_general(keys, queries, (((1,), (1,)), ((), ())), preferred_element_type=jnp.float32)
        scores = (scores * factor).reshape(2 * tokens // cols, cols, tokens) + bias[None]
        return scores.reshape(2 * tokens, tokens)

    def first_stage(h):
        for half in range(2):
            base = half * PER_HALF
            keys, values = block(h, base + 8, 2), block(h, base + 10, 2)
            for role in range(4):
                scores = scores_of(keys, block(h, base + role))
                dprobs = lax.dot_general(
                    values, block(h, base + 4 + role), (((1,), (1,)), ((), ())), preferred_element_type=jnp.float32
                )
                top = jnp.max(scores, axis=0, keepdims=True)
                weights = jnp.exp(scores - top)
                total = jnp.sum(weights, axis=0, keepdims=True)
                dots = jnp.sum(weights * dprobs, axis=0, keepdims=True)
                lanes = pl.ds(role * tokens, tokens)
                stat_out[h, half, 0:1, lanes] = top + jnp.log(total)
                stat_out[h, half, 1:2, lanes] = dots / total

    def second_stage(h):
        for half in range(2):
            base = half * PER_HALF
            keys, values = block(h, base + 8, 2), block(h, base + 10, 2)
            dk = jnp.zeros((2 * tokens, HEAD_DIM), jnp.float32)
            dv = jnp.zeros((2 * tokens, HEAD_DIM), jnp.float32)
            for role in range(4):
                lanes = pl.ds(role * tokens, tokens)
                mine, other = stat_out[h, half, 0:1, lanes], stat_in[h, half, 0:1, lanes]
                norm = jnp.maximum(mine, other) + jnp.log(1.0 + jnp.exp(-jnp.abs(mine - other)))
                row_dot = stat_out[h, half, 1:2, lanes] * jnp.exp(mine - norm)
                row_dot += stat_in[h, half, 1:2, lanes] * jnp.exp(other - norm)
                queries, grads = block(h, base + role), block(h, base + 4 + role)
                probs = jnp.exp(scores_of(keys, queries) - norm)
                dprobs = lax.dot_general(
                    values, grads, (((1,), (1,)), ((), ())), preferred_element_type=jnp.float32
                )
                dscores = (probs * (dprobs - row_dot) * factor).astype(jnp.bfloat16)
                dv += jnp.dot(probs.astype(jnp.bfloat16), grads, preferred_element_type=jnp.float32)
                dk += jnp.dot(dscores, queries, preferred_element_type=jnp.float32)
                dq = lax.dot_general(dscores, keys, (((0,), (0,)), ((), ())), preferred_element_type=jnp.float32)
                dq_part[h, half, role] = dq.astype(jnp.bfloat16).reshape(fh, rh, cols, HEAD_DIM)
            for kind, (ref, total) in enumerate(((dk_ref, dk), (dv_ref, dv))):
                total = total.astype(jnp.bfloat16).reshape(2, fh, rh, cols, HEAD_DIM)
                put(ref, half, 1, h, total[0])
                dkv[h, kind, half] = total[1]

    ahead = AHEAD + 2 * (seam_before + seam_after)

    def send_first(h, carry):
        send_inputs(h)
        return carry

    lax.fori_loop(0, ahead, send_first, 0)

    def step(i, carry):
        @pl.when(i < heads)
        def _():
            wait_bytes(blocks.at[i, pl.ds(0, 8)], load_sem.at[i])
            wait_bytes(blocks.at[i, pl.ds(0, 16)], fwd_recv.at[i])

        @pl.when(i + ahead < heads)
        def _():
            send_inputs(i + ahead)

        @pl.when(i > LAG)
        def _():
            send_outputs(i - LAG - 1)

        @pl.when(i < heads)
        def _():
            first_stage(i)

        @pl.when((i >= LAG) & (i < heads + LAG))
        def _():
            wait_bytes(stat_in.at[i - LAG], stat_recv.at[i - LAG])
            second_stage(i - LAG)

        @pl.when(i < heads)
        def _():
            send_stats(i)

        return carry

    lax.fori_loop(0, heads + LAG + 1, step, 0)

    def finish(h, carry):
        wait_bytes(dq_in.at[h], dq_recv.at[h])
        own = dq_part.at[h]
        for half, late_rows, first, second in (
            (1, 0, dq_in.at[h, 0], dq_in.at[h, 1]),
            (0, 0, dq_in.at[h, 2], dq_in.at[h, 3]),
            (1, 1, dq_in.at[h, 4], own.at[1, 0]),
            (0, 1, dq_in.at[h, 5], own.at[0, 2]),
        ):
            total = first[...].astype(jnp.float32) + second[...].astype(jnp.float32)
            put(dq_ref, half, late_rows, h, total.astype(jnp.bfloat16))
        return carry

    lax.fori_loop(0, heads, finish, 0)

    def drain(h, carry):
        wait_bytes(blocks.at[h, pl.ds(0, 16)], fwd_send.at[h])
        wait_bytes(stat_out.at[h], stat_send.at[h])
        wait_bytes(blocks.at[h, pl.ds(0, 10)], out_send.at[h])
        wait_bytes(blocks.at[h, pl.ds(0, 4)], dkv_recv.at[h])
        return carry

    lax.fori_loop(0, heads, drain, 0)


def write_out(*refs):
    sources, targets, sem = refs[:3], refs[3:6], refs[6]
    copies = [
        pltpu.make_async_copy(source.at[frame], target.at[frame], sem.at[i, frame])
        for i, (source, target) in enumerate(zip(sources, targets))
        for frame in range(source.shape[0])
    ]
    for copy in copies:
        copy.start()
    for copy in copies:
        copy.wait()


def solution(mesh):
    tm, rows = mesh.shape["tm"], mesh.shape["rows"]

    def shards(queries, keys, values, out_grad):
        frames, rows_here, cols, features = queries.shape
        heads = features // HEAD_DIM
        fh, rh = frames // 2, rows_here // 2
        tokens = fh * rh * cols
        quadrant = (fh, rh, cols, HEAD_DIM)
        bf16 = jnp.bfloat16
        hbm, vmem = pl.BlockSpec(memory_space=pl.ANY), pl.BlockSpec(memory_space=pltpu.VMEM)
        held = pltpu.VMEM(queries.shape, bf16)
        grads = pl.pallas_call(
            functools.partial(kernel, tm, rows),
            out_shape=(held, held, held),
            in_specs=[hbm] * 4,
            out_specs=(vmem, vmem, vmem),
            scratch_shapes=[
                pltpu.VMEM((heads, 2 * PER_HALF, *quadrant), bf16),
                pltpu.VMEM((heads, 2, 2, 4 * tokens), jnp.float32),
                pltpu.VMEM((heads, 2, 2, 4 * tokens), jnp.float32),
                pltpu.VMEM((heads, 2, 4, *quadrant), bf16),
                pltpu.VMEM((heads, 2, 2, *quadrant), bf16),
                pltpu.VMEM((heads, 6, *quadrant), bf16),
                pltpu.SemaphoreType.DMA((8, heads)),
            ],
            compiler_params=pltpu.CompilerParams(
                collective_id=0, has_side_effects=True, vmem_limit_bytes=57 * 1024 * 1024
            ),
        )(queries, keys, values, out_grad)
        out = jax.ShapeDtypeStruct(queries.shape, bf16)
        return pl.pallas_call(
            write_out,
            out_shape=(out, out, out),
            in_specs=[vmem] * 3,
            out_specs=(hbm, hbm, hbm),
            scratch_shapes=[pltpu.SemaphoreType.DMA((3, frames))],
            compiler_params=pltpu.CompilerParams(vmem_limit_bytes=4 * 1024 * 1024),
        )(*(pltpu.with_memory_space_constraint(grad, pltpu.VMEM) for grad in grads))

    spec = P("tm", "rows", None, None)
    return jax.shard_map(
        shards, mesh=mesh, in_specs=(spec,) * 4, out_specs=(spec,) * 3, check_vma=False
    )
```

```python
import functools
import math

import jax
import jax.numpy as jnp
from jax import lax
from jax.experimental import pallas as pl
from jax.experimental.pallas import tpu as pltpu
from jax.sharding import PartitionSpec as P

MESH = pl.DeviceIdType.MESH
HEAD_DIM = 128
WW = 8
AHEAD = 2
LAG = 5

PER_HALF = 12
OWN_ROLE = (2, 0)


def kernel(tm, rows, q_ref, k_ref, v_ref, g_ref, dq_ref, dk_ref, dv_ref, blocks, stat_out, stat_in, dq_part, dkv,
           dq_in, sems):
    t, r = lax.axis_index("tm"), lax.axis_index("rows")
    frames, rows_here, cols, features = q_ref.shape
    heads = features // HEAD_DIM
    fh, rh = frames // 2, rows_here // 2
    factor = 1.0 / math.sqrt(HEAD_DIM)
    side = rows // 2
    seam_before = 1 - (r % side + side - 1) // side
    seam_after = 1 - ((r + 1) % side + side - 1) // side
    tp, tn = (t + 1) % tm, (t + tm - 1) % tm
    first_way = (t + 1) // tm
    rp, rn = (r + 1) % rows, (r + rows - 1) % rows

    (fwd_send, fwd_recv, load_sem, stat_send, stat_recv, out_send, dq_recv, dkv_recv) = (
        sems.at[i] for i in range(8)
    )

    def quad(ref, late_frames, late_rows, h):
        return ref.at[
            pl.ds(late_frames * fh, fh),
            pl.ds(late_rows * rh, rh),
            :,
            pl.ds(pl.multiple_of(h * HEAD_DIM, HEAD_DIM), HEAD_DIM),
        ]

    def put(ref, late_frames, late_rows, h, value):
        lanes = pl.ds(pl.multiple_of(h * HEAD_DIM, HEAD_DIM), HEAD_DIM)
        ref[pl.ds(late_frames * fh, fh), pl.ds(late_rows * rh, rh), :, lanes] = value

    def send(src, dst, send_sem, recv_sem, device):
        pltpu.make_async_remote_copy(
            src_ref=src, dst_ref=dst, send_sem=send_sem, recv_sem=recv_sem, device_id=device, device_id_type=MESH
        ).start()

    def wait_bytes(ref, sem):
        pltpu.make_async_copy(ref, ref, sem).wait()

    barrier = pltpu.get_barrier_semaphore()
    senders = [(tp, r), (tn, r), (t, rp), (tp, rp), (tn, rp)]
    for device in senders:
        pl.semaphore_signal(barrier, inc=1, device_id=device, device_id_type=MESH)

    def load_own(h, carry):
        for half in range(2):
            base = half * PER_HALF
            role = OWN_ROLE[half]
            for ref, slot in ((q_ref, role), (g_ref, 4 + role), (k_ref, 8), (v_ref, 10)):
                pltpu.make_async_copy(quad(ref, half, 1, h), blocks.at[h, base + slot], load_sem.at[h]).start()
        return carry

    lax.fori_loop(0, heads, load_own, 0)
    pl.semaphore_wait(barrier, len(senders))

    def send_inputs(h):
        sem = (fwd_send.at[h], fwd_recv.at[h])
        for ref, off in ((q_ref, 0), (g_ref, 4)):
            send(quad(ref, 1, 1, h), blocks.at[h, off + 0], *sem, (tp, r))
            send(quad(ref, 0, 1, h), blocks.at[h, PER_HALF + off + 2], *sem, (tn, r))
            send(quad(ref, 1, 0, h), blocks.at[h, off + 1], *sem, (tp, rn))
            send(quad(ref, 0, 0, h), blocks.at[h, PER_HALF + off + 3], *sem, (tn, rn))
            send(quad(ref, 1, 0, h), blocks.at[h, PER_HALF + off + 1], *sem, (t, rn))
            send(quad(ref, 0, 0, h), blocks.at[h, off + 3], *sem, (t, rn))
        for ref, off in ((k_ref, 9), (v_ref, 11)):
            send(
                quad(ref, 1, 0, h),
                blocks.at[h, (1 - seam_before) * PER_HALF + off],
                *sem,
                ((t + seam_before) % tm, rn),
            )
            send(
                quad(ref, 0, 0, h),
                blocks.at[h, seam_before * PER_HALF + off],
                *sem,
                ((t + tm - seam_before) % tm, rn),
            )

    def send_stats(h):
        sem = (stat_send.at[h], stat_recv.at[h])
        send(stat_out.at[h, 1], stat_in.at[h, 0], *sem, (tp, r))
        send(stat_out.at[h, 0], stat_in.at[h, 1], *sem, (tn, r))

    def send_outputs(h):
        sem = (out_send.at[h], dq_recv.at[h])
        send(dq_part.at[h, 1, 1], dq_in.at[h, 0], *sem, (t, rp))
        send(dq_part.at[h, 0, 3], dq_in.at[h, 3], *sem, (t, rp))
        for way in (first_way, 1 - first_way):
            beside = (t + tm + 2 * way - 1) % tm
            send(dq_part.at[h, way, 1 + 2 * way], dq_in.at[h, 1 + way], *sem, (beside, rp))
            send(dq_part.at[h, way, 2 * way], dq_in.at[h, 4 + way], *sem, (beside, r))
        sem = (out_send.at[h], dkv_recv.at[h])
        for kind, ref in enumerate((dk_ref, dv_ref)):
            send(dkv.at[h, kind, 1], quad(ref, 1 - seam_after, 0, h), *sem, ((t + seam_after) % tm, rp))
            send(dkv.at[h, kind, 0], quad(ref, seam_after, 0, h), *sem, ((t + tm - seam_after) % tm, rp))

    key_col = lax.broadcasted_iota(jnp.int32, (cols, HEAD_DIM), 0)
    query_col = lax.broadcasted_iota(jnp.int32, (cols, HEAD_DIM), 1)
    shifted = cols - WW // 2
    apart = ((key_col + shifted) ^ (query_col + shifted)) & WW
    bias = jnp.where(apart == 0, 0.0, -1e30).astype(jnp.float32)

    tokens = fh * rh * cols

    def block(h, index, count=1):
        return blocks[h, pl.ds(index, count)].reshape(count * tokens, HEAD_DIM)

    def scores_of(keys, queries):
        scores = lax.dot_general(keys, queries, (((1,), (1,)), ((), ())), preferred_element_type=jnp.float32)
        scores = (scores * factor).reshape(2 * tokens // cols, cols, tokens) + bias[None]
        return scores.reshape(2 * tokens, tokens)

    def first_stage(h):
        for half in range(2):
            base = half * PER_HALF
            keys, values = block(h, base + 8, 2), block(h, base + 10, 2)
            for role in range(4):
                scores = scores_of(keys, block(h, base + role))
                dprobs = lax.dot_general(
                    values, block(h, base + 4 + role), (((1,), (1,)), ((), ())), preferred_element_type=jnp.float32
                )
                top = jnp.max(scores, axis=0, keepdims=True)
                weights = jnp.exp(scores - top)
                total = jnp.sum(weights, axis=0, keepdims=True)
                dots = jnp.sum(weights * dprobs, axis=0, keepdims=True)
                lanes = pl.ds(role * tokens, tokens)
                stat_out[h, half, 0:1, lanes] = top + jnp.log(total)
                stat_out[h, half, 1:2, lanes] = dots / total

    def second_stage(h):
        for half in range(2):
            base = half * PER_HALF
            keys, values = block(h, base + 8, 2), block(h, base + 10, 2)
            dk = jnp.zeros((2 * tokens, HEAD_DIM), jnp.float32)
            dv = jnp.zeros((2 * tokens, HEAD_DIM), jnp.float32)
            for role in range(4):
                lanes = pl.ds(role * tokens, tokens)
                mine, other = stat_out[h, half, 0:1, lanes], stat_in[h, half, 0:1, lanes]
                norm = jnp.maximum(mine, other) + jnp.log(1.0 + jnp.exp(-jnp.abs(mine - other)))
                row_dot = stat_out[h, half, 1:2, lanes] * jnp.exp(mine - norm)
                row_dot += stat_in[h, half, 1:2, lanes] * jnp.exp(other - norm)
                queries, grads = block(h, base + role), block(h, base + 4 + role)
                probs = jnp.exp(scores_of(keys, queries) - norm)
                dprobs = lax.dot_general(
                    values, grads, (((1,), (1,)), ((), ())), preferred_element_type=jnp.float32
                )
                dscores = (probs * (dprobs - row_dot) * factor).astype(jnp.bfloat16)
                dv += jnp.dot(probs.astype(jnp.bfloat16), grads, preferred_element_type=jnp.float32)
                dk += jnp.dot(dscores, queries, preferred_element_type=jnp.float32)
                dq = lax.dot_general(dscores, keys, (((0,), (0,)), ((), ())), preferred_element_type=jnp.float32)
                dq_part[h, half, role] = dq.astype(jnp.bfloat16).reshape(fh, rh, cols, HEAD_DIM)
            for kind, (ref, total) in enumerate(((dk_ref, dk), (dv_ref, dv))):
                total = total.astype(jnp.bfloat16).reshape(2, fh, rh, cols, HEAD_DIM)
                put(ref, half, 1, h, total[0])
                dkv[h, kind, half] = total[1]

    ahead = AHEAD + 2 * (seam_before + seam_after)

    def send_first(h, carry):
        send_inputs(h)
        return carry

    lax.fori_loop(0, ahead, send_first, 0)

    def step(i, carry):
        @pl.when(i < heads)
        def _():
            wait_bytes(blocks.at[i, pl.ds(0, 8)], load_sem.at[i])
            wait_bytes(blocks.at[i, pl.ds(0, 16)], fwd_recv.at[i])

        @pl.when(i + ahead < heads)
        def _():
            send_inputs(i + ahead)

        @pl.when(i > LAG)
        def _():
            send_outputs(i - LAG - 1)

        @pl.when(i < heads)
        def _():
            first_stage(i)

        @pl.when((i >= LAG) & (i < heads + LAG))
        def _():
            wait_bytes(stat_in.at[i - LAG], stat_recv.at[i - LAG])
            second_stage(i - LAG)

        @pl.when(i < heads)
        def _():
            send_stats(i)

        return carry

    lax.fori_loop(0, heads + LAG + 1, step, 0)

    def finish(h, carry):
        wait_bytes(dq_in.at[h], dq_recv.at[h])
        own = dq_part.at[h]
        for half, late_rows, first, second in (
            (1, 0, dq_in.at[h, 0], dq_in.at[h, 1]),
            (0, 0, dq_in.at[h, 2], dq_in.at[h, 3]),
            (1, 1, dq_in.at[h, 4], own.at[1, 0]),
            (0, 1, dq_in.at[h, 5], own.at[0, 2]),
        ):
            total = first[...].astype(jnp.float32) + second[...].astype(jnp.float32)
            put(dq_ref, half, late_rows, h, total.astype(jnp.bfloat16))
        return carry

    lax.fori_loop(0, heads, finish, 0)

    def drain(h, carry):
        wait_bytes(blocks.at[h, pl.ds(0, 16)], fwd_send.at[h])
        wait_bytes(stat_out.at[h], stat_send.at[h])
        wait_bytes(blocks.at[h, pl.ds(0, 10)], out_send.at[h])
        wait_bytes(blocks.at[h, pl.ds(0, 4)], dkv_recv.at[h])
        return carry

    lax.fori_loop(0, heads, drain, 0)


def write_out(*refs):
    sources, targets, sem = refs[:3], refs[3:6], refs[6]
    copies = [
        pltpu.make_async_copy(source.at[frame], target.at[frame], sem.at[i, frame])
        for i, (source, target) in enumerate(zip(sources, targets))
        for frame in range(source.shape[0])
    ]
    for copy in copies:
        copy.start()
    for copy in copies:
        copy.wait()


def solution(mesh):
    tm, rows = mesh.shape["tm"], mesh.shape["rows"]

    def shards(queries, keys, values, out_grad):
        frames, rows_here, cols, features = queries.shape
        heads = features // HEAD_DIM
        fh, rh = frames // 2, rows_here // 2
        tokens = fh * rh * cols
        quadrant = (fh, rh, cols, HEAD_DIM)
        bf16 = jnp.bfloat16
        hbm, vmem = pl.BlockSpec(memory_space=pl.ANY), pl.BlockSpec(memory_space=pltpu.VMEM)
        held = pltpu.VMEM(queries.shape, bf16)
        grads = pl.pallas_call(
            functools.partial(kernel, tm, rows),
            out_shape=(held, held, held),
            in_specs=[hbm] * 4,
            out_specs=(vmem, vmem, vmem),
            scratch_shapes=[
                pltpu.VMEM((heads, 2 * PER_HALF, *quadrant), bf16),
                pltpu.VMEM((heads, 2, 2, 4 * tokens), jnp.float32),
                pltpu.VMEM((heads, 2, 2, 4 * tokens), jnp.float32),
                pltpu.VMEM((heads, 2, 4, *quadrant), bf16),
                pltpu.VMEM((heads, 2, 2, *quadrant), bf16),
                pltpu.VMEM((heads, 6, *quadrant), bf16),
                pltpu.SemaphoreType.DMA((8, heads)),
            ],
            compiler_params=pltpu.CompilerParams(
                collective_id=0, has_side_effects=True, vmem_limit_bytes=57 * 1024 * 1024
            ),
        )(queries, keys, values, out_grad)
        out = jax.ShapeDtypeStruct(queries.shape, bf16)
        return pl.pallas_call(
            write_out,
            out_shape=(out, out, out),
            in_specs=[vmem] * 3,
            out_specs=(hbm, hbm, hbm),
            scratch_shapes=[pltpu.SemaphoreType.DMA((3, frames))],
            compiler_params=pltpu.CompilerParams(vmem_limit_bytes=4 * 1024 * 1024),
        )(*(pltpu.with_memory_space_constraint(grad, pltpu.VMEM) for grad in grads))

    spec = P("tm", "rows", None, None)
    return jax.shard_map(
        shards, mesh=mesh, in_specs=(spec,) * 4, out_specs=(spec,) * 3, check_vma=False
    )
```
